32 devices in a mesh: lon: 8 (over z, core), mem: 4 (over y, x).
Axes of the slice: x: 2, y: 2, z: 4, core: 2. Of those that a mesh axis runs over, the one named last changes fastest.
Arguments:
- alpha: bfloat16 [40, 128, 256, 128], P('mem', 'lon'), may hold values from -6 to 6
- ens_pert: bfloat16 [40, 128, 256, 128], P('mem', None, 'lon'), may hold values from -6 to 6
- vert_sqrt: bfloat16 [128, 128], replicated, may hold values from -0.5 to 0.5
- lat_sqrt: bfloat16 [128, 128], replicated, may hold values from -0.5 to 0.5
Outputs:
- increment: float32 [128, 256, 128], P('mem', 'lon')
The draws below stay inside these ranges and needn't reach their ends.
All inputs are finite; a program needn't handle non-finite values.
Results may differ from the reference program's by a relative error of at most 0.0042.
Values may be sent and summed in bfloat16 or wider, within the bound.
No kernel may reach another device: no remote copies, remote signals or barrier semaphores. Data moves between devices by JAX's collectives and lax.ppermute only.
A program may use at most 128 MiB of HBM per device.

```python
import math
import jax
import jax.numpy as jnp
from jax import lax

LEV = 128
LAT = 128
MEMBERS = 40
LON = 256


def block_scale(own_key, dims, pieces, low, high):
    gain = 1.0
    for dim, blocks in pieces:
        draws = jax.random.uniform(jax.random.fold_in(jax.random.fold_in(own_key, 6), dim), (blocks,), jnp.float32, low / len(pieces), high / len(pieces))
        gain = gain * jnp.repeat(jnp.exp(draws), dims[dim] // blocks).reshape((-1,) + (1,) * (len(dims) - 1 - dim))
    return gain


def bell_draw(stream_key, shape, deviation, limit, cuts=(), kind=jnp.bfloat16):
    gain = block_scale(stream_key, shape, cuts, -0.22, 0.18) if cuts else 1.0
    entries = jax.random.normal(stream_key, shape, jnp.float32) * deviation * gain
    return jnp.minimum(jnp.maximum(entries, -limit), limit).astype(kind)


def setup_inputs(seed: int = 0) -> dict:
    seeds = jax.random.split(jax.random.key(seed), 5)
    alpha = bell_draw(seeds[0], (MEMBERS, LEV, LON, LAT), 1.0, 6.0, ((0, 4), (1, 8)))
    ens_pert = bell_draw(seeds[1], (MEMBERS, LEV, LON, LAT), 1.0, 6.0, ((0, 4), (2, 8)))
    vert_sqrt = bell_draw(seeds[2], (LEV, LEV), LEV ** -0.5, 0.5)
    lat_sqrt = bell_draw(seeds[3], (LAT, LAT), LAT ** -0.5, 0.5)
    return {"alpha": alpha, "ens_pert": ens_pert, "vert_sqrt": vert_sqrt, "lat_sqrt": lat_sqrt}


def reference(alpha, ens_pert, vert_sqrt, lat_sqrt):
    factor = 1.0 / math.sqrt(MEMBERS)
    vert_full = vert_sqrt.astype(jnp.float32)
    lat_full = lat_sqrt.astype(jnp.float32)

    def member_step(total, pair):
        member_alpha, member_pert = pair
        vertical = jnp.einsum('kl,lxi->kxi', vert_full, member_alpha.astype(jnp.float32), precision=lax.Precision.HIGHEST).astype(jnp.bfloat16)
        localized = jnp.einsum('kxi,ij->kxj', vertical.astype(jnp.float32), lat_full, precision=lax.Precision.HIGHEST)
        return (total + member_pert.astype(jnp.float32) * localized, None)
    initial = jnp.zeros((LEV, LON, LAT), jnp.float32)
    total, unused = lax.scan(member_step, initial, (alpha, ens_pert))
    return total * factor
```

```python
import math

import jax
import jax.numpy as jnp
from jax import lax
from jax.experimental import pallas as pl
from jax.experimental.pallas import tpu as pltpu
from jax.sharding import PartitionSpec as P


def partner(index, step, count):
    if count & (count - 1) == 0:
        return index ^ step
    return lax.rem(step + count - index, count)


def swap(value, axis, step):
    count = lax.axis_size(axis)
    pairs = []
    for index in range(count):
        other = index ^ step if count & (count - 1) == 0 else (step - index) % count
        pairs.append((index, other))
    return lax.ppermute(value, axis, pairs)


def chunk_rows(total):
    return [8] * (total // 8 - 1) + [4, 4]


def relayout(array, own, windows, row, rows):
    members, levels, _, lats = array.shape
    block = 2 if members % 2 == 0 else 1
    shift = row % 8

    def body(own_ref, *refs):
        sources, outs, wide = refs[:len(windows)], refs[len(windows):-1], refs[-1]
        for source, out in zip(sources, outs):
            for member in range(block):
                wide[...] = source[member].astype(jnp.float32)
                for x in range(rows):
                    out[x, member] = wide[:, shift + x, :].astype(array.dtype)

    def source_spec(window):
        return pl.BlockSpec(
            (block, levels, 8, lats), lambda m, own: (m, 0, window(own) + row // 8, 0)
        )

    return pl.pallas_call(
        body,
        grid_spec=pltpu.PrefetchScalarGridSpec(
            num_scalar_prefetch=1,
            grid=(members // block,),
            in_specs=[source_spec(window) for window in windows],
            out_specs=[
                pl.BlockSpec((rows, block, levels, lats), lambda m, own: (0, m, 0, 0))
            ] * len(windows),
            scratch_shapes=[pltpu.VMEM((levels, 8, lats), jnp.float32)],
        ),
        out_shape=[
            jax.ShapeDtypeStruct((rows, members, levels, lats), array.dtype)
        ] * len(windows),
        cost_estimate=pl.CostEstimate(
            flops=len(windows) * members * levels * lats * rows,
            bytes_accessed=len(windows) * members * levels * lats * rows * 4,
            transcendentals=0,
        ),
    )(own, *[array] * len(windows))


def weigh_kernel(groups, members, own_ref, vert_ref, lat_ref, pert_ref, *refs):
    pieces, outs, total = refs[:-groups - 1], refs[-groups - 1:-1], refs[-1]
    half = lat_ref.shape[0] // 2

    def columns(member):
        return jnp.concatenate([piece[0, member] for piece in pieces], axis=0)

    for member in range(0, members, 2):
        pair = min(2, members - member)
        field = columns(member)
        if pair == 2:
            field = jnp.concatenate([field, columns(member + 1)], axis=1)
        vertical = jnp.dot(
            vert_ref[...], field, preferred_element_type=jnp.float32
        ).astype(jnp.bfloat16)
        weights = lat_ref[...] if pair == 2 else lat_ref[:half, :half]
        localized = jnp.dot(vertical, weights, preferred_element_type=jnp.float32)
        part = pert_ref[0, member].astype(jnp.float32) * localized[:, :half]
        if pair == 2:
            part += pert_ref[0, member + 1].astype(jnp.float32) * localized[:, half:]
        if member == 0:
            total[...] = part
        else:
            total[...] += part
    levels = total.shape[0] // groups
    for step, out in enumerate(outs):
        start = partner(own_ref[1], step, groups) * levels
        out[0] = total[pl.ds(pl.multiple_of(start, levels), levels), :]


def weigh(own, vert, lat_pair, pert, row, rows, pieces, groups):
    members, levels, lats = pert.shape[1:]
    part = levels // groups
    piece_spec = pl.BlockSpec((1,) + pieces[0].shape[1:], lambda x, own: (x, 0, 0, 0))
    whole = lambda x, own: (0, 0)
    grid_spec = pltpu.PrefetchScalarGridSpec(
        num_scalar_prefetch=1,
        grid=(rows,),
        in_specs=[
            pl.BlockSpec(vert.shape, whole),
            pl.BlockSpec(lat_pair.shape, whole),
            pl.BlockSpec((1, members, levels, lats), lambda x, own: (x + row, 0, 0, 0)),
        ]
        + [piece_spec] * len(pieces),
        out_specs=[pl.BlockSpec((1, part, lats), lambda x, own: (x, 0, 0))] * groups,
        scratch_shapes=[pltpu.VMEM((levels, lats), jnp.float32)],
    )

    def body(*refs):
        weigh_kernel(groups, members, *refs)

    return pl.pallas_call(
        body,
        grid_spec=grid_spec,
        out_shape=[jax.ShapeDtypeStruct((rows, part, lats), jnp.float32)] * groups,
        cost_estimate=pl.CostEstimate(
            flops=rows * members * levels * lats * (levels + lats) * 2,
            bytes_accessed=rows * members * levels * lats * 4,
            transcendentals=0,
        ),
    )(own, vert, lat_pair, pert, *pieces)


def finish(factor, parts, longitudes):
    levels, lats = parts[0][0].shape[1:]
    count = len(parts[0])

    def body(*refs):
        out = refs[-1]
        row = 0
        for chunk in range(len(parts)):
            pieces = refs[chunk * count:(chunk + 1) * count]
            for x in range(pieces[0].shape[0]):
                value = pieces[0][x]
                for piece in pieces[1:]:
                    value += piece[x]
                out[:, row, :] = value * factor
                row += 1

    return pl.pallas_call(
        body,
        out_shape=jax.ShapeDtypeStruct((levels, longitudes, lats), jnp.float32),
    )(*[piece for chunk in parts for piece in chunk])


def local(alpha, ens_pert, vert_sqrt, lat_sqrt):
    members, own_levels, _, lats = alpha.shape
    levels, longitudes = ens_pert.shape[1:3]
    count, groups = lax.axis_size("lon"), lax.axis_size("mem")
    me, group = lax.axis_index("lon"), lax.axis_index("mem")
    factor = 1.0 / math.sqrt(members * groups)

    own = jnp.stack([me, group]).astype(jnp.int32)
    sizes = chunk_rows(longitudes)
    starts = [sum(sizes[:index]) for index in range(len(sizes))]

    def window(step):
        return lambda own: partner(own[0], step, count) * (longitudes // 8)

    held = []
    for chunk, (row, rows) in enumerate(zip(starts, sizes)):
        with jax.named_scope(f"pack{chunk}"):
            packed = relayout(alpha, own, [window(step) for step in range(count)], row, rows)
        pieces = [packed[0]]
        for step in range(1, count):
            with jax.named_scope(f"go{chunk}_{step}"):
                pieces.append(swap(packed[step], "lon", step))
        held.append(pieces)

    level = lax.broadcasted_iota(jnp.int32, (levels, levels), 0)
    place = lax.broadcasted_iota(jnp.int32, (levels, levels), 1)
    source = partner(me, place // own_levels, count) * own_levels + place % own_levels
    vert = jnp.dot(
        vert_sqrt, (level == source).astype(vert_sqrt.dtype), preferred_element_type=jnp.float32
    ).astype(vert_sqrt.dtype)
    zero = jnp.zeros_like(lat_sqrt)
    lat_pair = jnp.block([[lat_sqrt, zero], [zero, lat_sqrt]])
    perts = []
    for row in range(0, longitudes, 8):
        with jax.named_scope(f"pert{row // 8}"):
            perts += relayout(ens_pert, own, [lambda own: 0], row, 8)

    parts = []
    for row, rows, pieces in zip(starts, sizes, held):
        with jax.named_scope("weigh"):
            sums = weigh(own, vert, lat_pair, perts[row // 8], row % 8, rows, pieces, groups)
        summed = [sums[0]]
        for step in range(1, groups):
            with jax.named_scope(f"sum{row}_{step}"):
                summed.append(swap(sums[step], "mem", step))
        parts.append(summed)
    return finish(factor, parts, longitudes)


def solution(mesh):
    placed = (P("mem", "lon", None, None), P("mem", None, "lon", None), P(), P())
    return jax.shard_map(
        local, mesh=mesh, in_specs=placed, out_specs=P("mem", "lon", None), check_vma=False
    )
```
